32 devices in a mesh: band: 2 (over x), tm: 16 (over z, y, core).
Axes of the slice: x: 2, y: 2, z: 4, core: 2. Of those that a mesh axis runs over, the one named last changes fastest.
Arguments:
- volts: int32 [8, 2, 3145728], P('band', None, 'tm'), parts along dimension 0, may hold values from -128 to 127, as said below
- taps: float32 [16, 4096], replicated, may hold values from -0.024 to 0.024
- pairs: int32 [4, 2], replicated, may hold values from 0 to 3, as said below
Outputs:
- coherence: float32 [8, 4096], P('band'), parts along dimension 0
- normalized: float32 [2, 8, 768, 4096], P(None, 'band', 'tm'), parts along dimension 1
The draws below stay inside these ranges and needn't reach their ends.
There are 2 independent parts, one for each index of `band`. The reference program is written for one: setup_inputs(seed, part) draws one part's arguments, and reference() takes and returns one part's arrays. A program takes and returns all parts, laid end to end along the dimension named above; an argument that names none is the same for every part. Nothing has to cross between parts.
Inputs may be any that keep to these rules, and one draw needn't show every extreme that they name: `volts`: every sample is a whole number of the int8 range. Each pair names a stream of the first antenna (0 or 1) and then one of the second antenna (2 or 3); the four pairs are distinct.
All inputs are finite; a program needn't handle non-finite values.
Results may differ from the reference program's by a relative error of at most 0.000067.
Values sent between devices are 32-bit elements; how exact they have to be, the bound alone decides.
No kernel may reach another device: no remote copies, remote signals or barrier semaphores. Data moves between devices by JAX's collectives and lax.ppermute only.
A program may use at most 128 MiB of HBM per device.

```python
import jax
import jax.numpy as jnp
from jax import lax

STREAMS = 4
TAPS = 16
CHANNELS = 4096
FRAMES = 768
SAMPLES = 3145728


def draw_volts(key, part):
    common_key = jax.random.fold_in(key, 11)
    noise_key = jax.random.fold_in(key, 12)
    weight_key = jax.random.fold_in(key, 13)
    delay_key = jax.random.fold_in(key, 14)
    common = jax.random.randint(common_key, (2, SAMPLES), -64, 64)
    noise = jax.random.randint(noise_key, (STREAMS, 2, SAMPLES), -64, 64)
    weights = jax.random.randint(weight_key, (STREAMS,), 0, 2)
    delay = jax.random.randint(delay_key, (), 0, 8)
    delayed = jnp.roll(common, delay, axis=1)
    antenna = (jnp.arange(STREAMS) >= 2).astype(jnp.int32)
    chosen = jnp.where(antenna[:, None, None] == 1, delayed[None], common[None])
    return (noise + weights[:, None, None] * chosen).astype(jnp.int32)


def draw_pairs(key, part):
    order = jax.random.permutation(jax.random.fold_in(key, 21), 4)
    return jnp.stack([order // 2, 2 + order % 2], axis=1).astype(jnp.int32)


def gaussian(key, dims, width, most, held_as=jnp.bfloat16):
    return jnp.clip(width * jax.random.normal(key, dims, jnp.float32), -most, most).astype(held_as)


def setup_inputs(seed: int = 0, part: int = 0) -> dict:
    seeds = jax.random.split(jax.random.key(seed), 4)
    part_keys = jax.random.split(jax.random.fold_in(seeds[3], part), 4)
    volts = draw_volts(jax.random.fold_in(jax.random.fold_in(seeds[3], part), 71), part)
    taps = gaussian(seeds[1], (TAPS, CHANNELS), 0.004, 0.024, jnp.float32)
    pairs = draw_pairs(jax.random.fold_in(seeds[3], 71), part)
    return dict(volts=volts, taps=taps, pairs=pairs)


def reference(volts, taps, pairs):
    samples = volts.astype(jnp.float32).reshape(STREAMS, 2, FRAMES, CHANNELS)
    padded = jnp.pad(samples, ((0, 0), (0, 0), (TAPS - 1, 0), (0, 0)))
    filtered = jnp.zeros((STREAMS, 2, FRAMES, CHANNELS), jnp.float32)
    for tap_index in range(TAPS):
        begin = TAPS - 1 - tap_index
        filtered = filtered + taps[tap_index] * padded[:, :, begin:begin + FRAMES]
    spectra = jnp.fft.fft(filtered[:, 0] + 1j * filtered[:, 1], axis=-1) / jnp.sqrt(jnp.float32(CHANNELS))
    real_part = jnp.real(spectra).astype(jnp.float32)
    imag_part = jnp.imag(spectra).astype(jnp.float32)
    auto = lax.optimization_barrier(jnp.sum(real_part * real_part + imag_part * imag_part, axis=1)) / FRAMES
    first = pairs[:, 0]
    second = pairs[:, 1]
    left_re = real_part[first]
    left_im = imag_part[first]
    right_re = real_part[second]
    right_im = imag_part[second]
    prod_re = left_re * right_re + left_im * right_im
    prod_im = left_im * right_re - left_re * right_im
    cross_re = lax.optimization_barrier(jnp.sum(prod_re, axis=1)) / FRAMES
    cross_im = lax.optimization_barrier(jnp.sum(prod_im, axis=1)) / FRAMES
    denom = (auto[first] + 1e-06) * (auto[second] + 1e-06)
    coherence = (cross_re * cross_re + cross_im * cross_im) / denom
    factor = 1.0 / jnp.sqrt(denom)
    normalized = jnp.stack([prod_re * factor[:, None], prod_im * factor[:, None]])
    return (coherence, normalized)
```

```python
import functools

import jax
import jax.numpy as jnp
import numpy as np
from jax import lax
from jax.experimental import pallas as pl
from jax.experimental.pallas import tpu as pltpu
from jax.sharding import PartitionSpec as P

LANES = 128
GROUP = 8
PITCH = 40


def shifted(array, axis, by):
    devices = lax.axis_size(axis)
    pairs = [(i, i + by) for i in range(devices) if 0 <= i + by < devices]
    return lax.ppermute(array, axis, pairs)


def halves(matrix):
    matrix = np.asarray(matrix, np.float32)
    high = matrix.astype(jnp.bfloat16)
    low = (matrix - high.astype(np.float32)).astype(jnp.bfloat16)
    return high, low


@functools.lru_cache(maxsize=None)
def tables(channels):
    radix = channels // LANES
    per_row = LANES // radix
    i = np.arange(radix)
    angle = 2.0 * np.pi * ((i[:, None] * i[None, :]) % radix) / radix
    first = np.zeros((2, radix, radix, 2))
    first[0, :, :, 0] = np.cos(angle)
    first[0, :, :, 1] = np.sin(angle)
    first[1, :, :, 0] = -np.sin(angle)
    first[1, :, :, 1] = np.cos(angle)
    high, low = halves(first.reshape(2 * radix, 2 * radix))
    left = np.concatenate([high, high, low, low], axis=1)
    j = np.arange(LANES)
    twist = 2.0 * np.pi * ((i[:, None] * j[None, :]) % channels) / channels
    twist = np.stack([np.cos(twist), np.sin(twist)]).astype(np.float32)
    g = np.arange(per_row)
    s = np.arange(radix)
    b = (per_row * s[None, :] + g[:, None]).reshape(LANES)
    angle = 2.0 * np.pi * ((j[:, None] * b[None, :]) % LANES) / LANES
    cos, sin = np.cos(angle), np.sin(angle)
    second = np.block([[cos, -sin], [sin, cos]]) / np.sqrt(channels)
    high, low = halves(second)
    right = np.concatenate([high, high, low], axis=0)
    return left, twist, right


def natural(block, radix):
    turned = block.T
    per_row = LANES // radix
    return [
        jnp.concatenate(
            [turned[g * radix : (g + 1) * radix, f * radix : (f + 1) * radix] for g in range(per_row)],
            axis=1,
        )
        for f in range(per_row)
    ]


def kernel(pairs, taps, left, twist, right, acc_in, old2, old1, cur, *rest, skip, finish, aliased):
    out, sums, filt, spec, acc, nat = rest[1:] if aliased else rest
    streams = cur.shape[0]
    count = pairs.shape[0]
    n_taps, rows, _ = taps.shape
    radix = rows // 2
    step = pl.program_id(0)
    last = pl.num_programs(0) - 1
    per_row = LANES // radix
    behind1 = GROUP
    behind2 = n_taps - 1 - GROUP
    tiles = rows // 8

    @pl.when(step == 0)
    def _():
        acc[...] = acc_in[...]

    def filter_tile(index, carry):
        s = index // tiles
        q = pl.multiple_of((index % tiles) * 8, 8)
        coef = [taps[t, pl.ds(q, 8), :] for t in range(n_taps)]
        total = [None] * GROUP
        for w in range(n_taps - 1 + GROUP):
            if w < behind2:
                x = old2[s, pl.ds((w + skip) * rows + q, 8), :]
            elif w < behind2 + behind1:
                x = old1[s, pl.ds((w - behind2) * rows + q, 8), :]
            else:
                x = cur[s, pl.ds((w - behind2 - behind1) * rows + q, 8), :]
            x = x.astype(jnp.float32)
            for m in range(GROUP):
                t = m + n_taps - 1 - w
                if 0 <= t < n_taps:
                    term = coef[t] * x
                    total[m] = term if total[m] is None else total[m] + term
        for m in range(GROUP):
            filt[s, pl.ds(m * rows + q, 8), :] = total[m]
        return carry

    lax.fori_loop(0, streams * tiles, filter_tile, 0)

    def transform(s, carry):
        turned = []
        for pair in range(GROUP // 2):
            columns = []
            for f in (2 * pair, 2 * pair + 1):
                x = filt[s, f * rows : (f + 1) * rows, :]
                high = x.astype(jnp.bfloat16)
                low = (x - high.astype(jnp.float32)).astype(jnp.bfloat16)
                columns.append(jnp.concatenate([high, low, high, low], axis=0))
            y = jnp.dot(
                left[...], jnp.concatenate(columns, axis=1), preferred_element_type=jnp.float32
            )
            for f in range(2):
                re = y[:radix, f * LANES : (f + 1) * LANES]
                im = y[radix:, f * LANES : (f + 1) * LANES]
                z = jnp.concatenate(
                    [re * twist[0] + im * twist[1], im * twist[0] - re * twist[1]], axis=1
                )
                turned.append(z)
        z = jnp.concatenate(turned, axis=0)
        high = z.astype(jnp.bfloat16)
        low = (z - high.astype(jnp.float32)).astype(jnp.bfloat16)
        full = jnp.dot(
            jnp.concatenate([high, low, high], axis=1),
            right[...],
            preferred_element_type=jnp.float32,
        )
        spec[s] = full
        power = full[:, :LANES] * full[:, :LANES] + full[:, LANES:] * full[:, LANES:]
        acc[s] += power.reshape(GROUP, radix, LANES).sum(axis=0)
        return carry

    lax.fori_loop(0, streams, transform, 0)

    def correlate(p, carry):
        a = pairs[p, 0]
        b = pairs[p, 1]
        for half in range(GROUP // per_row):
            span = slice(half * LANES, (half + 1) * LANES)
            a_re = spec[a, span, :LANES]
            a_im = spec[a, span, LANES:]
            b_re = spec[b, span, :LANES]
            b_im = spec[b, span, LANES:]
            for part in range(2):
                if part == 0:
                    prod = a_re * b_re + a_im * b_im
                else:
                    prod = a_im * b_re - a_re * b_im
                acc[streams + part * count + p] += prod.reshape(per_row, radix, LANES).sum(axis=0)
                for f, block in enumerate(natural(prod, radix)):
                    start = (half * per_row + f) * PITCH
                    nat[part, start : start + radix, :] = block
        for part in range(2):
            for s in range(radix):
                out[part, p, :, s * LANES : (s + 1) * LANES] = nat[
                    part, pl.ds(s, GROUP, stride=PITCH), :
                ]
        return carry

    lax.fori_loop(0, count, correlate, 0)

    @pl.when(step == last)
    def _():
        if finish:
            for first in range(0, streams + 2 * count, per_row):
                block = acc[first : first + per_row].reshape(LANES, LANES)
                for f, piece in enumerate(natural(block, radix)):
                    sums[first + f] = piece
        else:
            sums[...] = acc[...]


def channelize(consts, acc_in, old2, old1, cur, base, steps, skip, finish, spectra, shape):
    streams = cur[0].shape[0]
    rows = consts[1].shape[1]
    radix = rows // 2
    size = GROUP * rows

    def block(entry):
        array, first = entry
        return pl.BlockSpec(
            (streams, min(size, array.shape[1]), LANES), lambda i: (0, first + i, 0)
        )

    whole = pl.BlockSpec(memory_space=pltpu.VMEM)
    ins = [pl.BlockSpec(memory_space=pltpu.SMEM)] + [whole] * 5
    ins += [block(old2), block(old1), block(cur)]
    args = list(consts) + [acc_in, old2[0], old1[0], cur[0]]
    aliases = {}
    if spectra is not None:
        ins.append(pl.BlockSpec(memory_space=pl.ANY))
        args.append(spectra)
        aliases = {len(args) - 1: 0}
    parts, count, frames, channels = shape
    return pl.pallas_call(
        functools.partial(kernel, skip=skip, finish=finish, aliased=spectra is not None),
        grid=(steps,),
        in_specs=ins,
        out_specs=[
            pl.BlockSpec((parts, count, GROUP, channels), lambda i: (0, 0, base + i, 0)),
            whole,
        ],
        out_shape=[
            jax.ShapeDtypeStruct(shape, jnp.float32),
            jax.ShapeDtypeStruct(acc_in.shape, jnp.float32),
        ],
        scratch_shapes=[
            pltpu.VMEM((streams, size, LANES), jnp.float32),
            pltpu.VMEM((streams, GROUP * radix, 2 * LANES), jnp.float32),
            pltpu.VMEM(acc_in.shape, jnp.float32),
            pltpu.VMEM((2, GROUP * PITCH, LANES), jnp.float32),
        ],
        input_output_aliases=aliases,
        compiler_params=pltpu.CompilerParams(vmem_limit_bytes=40 << 20),
        name="channelize",
    )(*args)


def scale_kernel(factor, prod, out):
    for p in range(prod.shape[1]):
        out[:, p] = prod[:, p] * factor[p : p + 1, :][None]


def rescale(products, factor):
    parts, count, frames, channels = products.shape
    spec = pl.BlockSpec((parts, count, GROUP, channels), lambda i: (0, 0, i, 0))
    return pl.pallas_call(
        scale_kernel,
        grid=(frames // GROUP,),
        in_specs=[pl.BlockSpec(memory_space=pltpu.VMEM), spec],
        out_specs=spec,
        out_shape=jax.ShapeDtypeStruct(products.shape, jnp.float32),
        input_output_aliases={1: 0},
        name="rescale",
    )(factor, products)


def on_device(volts, taps, pairs):
    streams, comps, local = volts.shape
    n_taps, channels = taps.shape
    count = pairs.shape[0]
    edge = n_taps - 1
    frames = local // channels
    radix = channels // LANES
    rows = comps * radix
    devices = lax.axis_size("tm")
    samples = volts.reshape(streams, comps, local // LANES, LANES)
    samples = samples.transpose(0, 2, 1, 3).reshape(streams, frames * rows, LANES)
    near = shifted(samples[:, (frames - GROUP) * rows :], "tm", 1)
    far = shifted(samples[:, (frames - edge) * rows : (frames - GROUP) * rows], "tm", 1)
    left, twist, right = tables(channels)
    coef = jnp.repeat(taps.reshape(n_taps, radix, LANES), comps, axis=1)
    consts = (pairs, coef, jnp.asarray(left), jnp.asarray(twist), jnp.asarray(right))
    acc = jnp.zeros((streams + 2 * count, radix, LANES), jnp.float32)
    shape = (2, count, frames, channels)
    rest = frames // GROUP - 2
    spectra, acc = channelize(
        consts, acc, (samples, 0), (samples, 1), (samples, 2), 2, rest, 1, False, None, shape
    )
    spectra, acc = channelize(
        consts, acc, (near, 0), (samples, 0), (samples, 1), 1, 1, 1, False, spectra, shape
    )
    spectra, acc = channelize(
        consts, acc, (far, 0), (near, 0), (samples, 0), 0, 1, 0, True, spectra, shape
    )
    sums = acc.reshape(streams + 2 * count, devices, channels // devices)
    sums = lax.all_to_all(sums.transpose(1, 0, 2), "tm", 0, 0)
    mean = jnp.sum(sums, axis=0) / (frames * devices)
    auto = mean[:streams] + 1e-06
    cross_re = mean[streams : streams + count]
    cross_im = mean[streams + count :]
    denom = jnp.take(auto, pairs[:, 0], axis=0) * jnp.take(auto, pairs[:, 1], axis=0)
    coherence = (cross_re * cross_re + cross_im * cross_im) / denom
    factor = 1.0 / jnp.sqrt(denom)
    both = lax.all_gather(jnp.concatenate([coherence, factor]), "tm", axis=0)
    both = both.transpose(1, 0, 2).reshape(2 * count, channels)
    return (both[:count], rescale(spectra, both[count:]))


def solution(mesh):
    return jax.shard_map(
        on_device,
        mesh=mesh,
        in_specs=(P("band", None, "tm"), P(), P()),
        out_specs=(P("band", None), P(None, "band", "tm", None)),
        check_vma=False,
    )
```

```python
import functools

import jax
import jax.numpy as jnp
import numpy as np
from jax import lax
from jax.experimental import pallas as pl
from jax.experimental.pallas import tpu as pltpu
from jax.sharding import PartitionSpec as P

LANES = 128
GROUP = 8
PITCH = 40


def shifted(array, axis, by):
    devices = lax.axis_size(axis)
    pairs = [(i, i + by) for i in range(devices) if 0 <= i + by < devices]
    return lax.ppermute(array, axis, pairs)


def halves(matrix):
    matrix = np.asarray(matrix, np.float32)
    high = matrix.astype(jnp.bfloat16)
    low = (matrix - high.astype(np.float32)).astype(jnp.bfloat16)
    return high, low


@functools.lru_cache(maxsize=None)
def tables(channels):
    radix = channels // LANES
    per_row = LANES // radix
    i = np.arange(radix)
    angle = 2.0 * np.pi * ((i[:, None] * i[None, :]) % radix) / radix
    first = np.zeros((2, radix, radix, 2))
    first[0, :, :, 0] = np.cos(angle)
    first[0, :, :, 1] = np.sin(angle)
    first[1, :, :, 0] = -np.sin(angle)
    first[1, :, :, 1] = np.cos(angle)
    high, low = halves(first.reshape(2 * radix, 2 * radix))
    left = np.concatenate([high, high, low, low], axis=1)
    j = np.arange(LANES)
    twist = 2.0 * np.pi * ((i[:, None] * j[None, :]) % channels) / channels
    twist = np.stack([np.cos(twist), np.sin(twist)]).astype(np.float32)
    g = np.arange(per_row)
    s = np.arange(radix)
    b = (per_row * s[None, :] + g[:, None]).reshape(LANES)
    angle = 2.0 * np.pi * ((j[:, None] * b[None, :]) % LANES) / LANES
    cos, sin = np.cos(angle), np.sin(angle)
    second = np.block([[cos, -sin], [sin, cos]]) / np.sqrt(channels)
    high, low = halves(second)
    right = np.concatenate([high, high, low], axis=0)
    return left, twist, right


def natural(block, radix):
    turned = block.T
    per_row = LANES // radix
    return [
        jnp.concatenate(
            [turned[g * radix : (g + 1) * radix, f * radix : (f + 1) * radix] for g in range(per_row)],
            axis=1,
        )
        for f in range(per_row)
    ]


def cut_kernel(block2, block1, far, near):
    far[...] = block2[:, block2.shape[1] - far.shape[1] :, :]
    near[...] = block1[...]


def cut(samples, rows, edge):
    streams, total, lanes = samples.shape
    size = GROUP * rows
    blocks = total // size
    whole = pl.BlockSpec(memory_space=pltpu.VMEM)
    return pl.pallas_call(
        cut_kernel,
        grid=(1,),
        in_specs=[
            pl.BlockSpec((streams, size, lanes), lambda i: (0, blocks - 2, 0)),
            pl.BlockSpec((streams, size, lanes), lambda i: (0, blocks - 1, 0)),
        ],
        out_specs=[whole, whole],
        out_shape=[
            jax.ShapeDtypeStruct((streams, (edge - GROUP) * rows, lanes), samples.dtype),
            jax.ShapeDtypeStruct((streams, size, lanes), samples.dtype),
        ],
        compiler_params=pltpu.CompilerParams(vmem_limit_bytes=58 << 20),
        name="cut",
    )(samples, samples)


def kernel(pairs, taps, left, twist, right, acc_in, old2, old1, cur, spec, sums, filt, acc, *, skip, finish):
    streams = cur.shape[0]
    count = pairs.shape[0]
    n_taps, rows, _ = taps.shape
    radix = rows // 2
    step = pl.program_id(0)
    last = pl.num_programs(0) - 1
    per_row = LANES // radix
    behind1 = GROUP
    behind2 = n_taps - 1 - GROUP
    tiles = rows // 8

    @pl.when(step == 0)
    def _():
        acc[...] = acc_in[...]

    def filter_tile(index, carry):
        s = index // tiles
        q = pl.multiple_of((index % tiles) * 8, 8)
        coef = [taps[t, pl.ds(q, 8), :] for t in range(n_taps)]
        total = [None] * GROUP
        for w in range(n_taps - 1 + GROUP):
            if w < behind2:
                x = old2[s, pl.ds((w + skip) * rows + q, 8), :]
            elif w < behind2 + behind1:
                x = old1[s, pl.ds((w - behind2) * rows + q, 8), :]
            else:
                x = cur[s, pl.ds((w - behind2 - behind1) * rows + q, 8), :]
            x = x.astype(jnp.float32)
            for m in range(GROUP):
                t = m + n_taps - 1 - w
                if 0 <= t < n_taps:
                    term = coef[t] * x
                    total[m] = term if total[m] is None else total[m] + term
        for m in range(GROUP):
            filt[s, pl.ds(m * rows + q, 8), :] = total[m]
        return carry

    lax.fori_loop(0, streams * tiles, filter_tile, 0)

    def transform(s, carry):
        turned = []
        for pair in range(GROUP // 2):
            columns = []
            for f in (2 * pair, 2 * pair + 1):
                x = filt[s, f * rows : (f + 1) * rows, :]
                high = x.astype(jnp.bfloat16)
                low = (x - high.astype(jnp.float32)).astype(jnp.bfloat16)
                columns.append(jnp.concatenate([high, low, high, low], axis=0))
            y = jnp.dot(
                left[...], jnp.concatenate(columns, axis=1), preferred_element_type=jnp.float32
            )
            for f in range(2):
                re = y[:radix, f * LANES : (f + 1) * LANES]
                im = y[radix:, f * LANES : (f + 1) * LANES]
                z = jnp.concatenate(
                    [re * twist[0] + im * twist[1], im * twist[0] - re * twist[1]], axis=1
                )
                turned.append(z)
        z = jnp.concatenate(turned, axis=0)
        high = z.astype(jnp.bfloat16)
        low = (z - high.astype(jnp.float32)).astype(jnp.bfloat16)
        full = jnp.dot(
            jnp.concatenate([high, low, high], axis=1),
            right[...],
            preferred_element_type=jnp.float32,
        )
        spec[s] = full
        power = full[:, :LANES] * full[:, :LANES] + full[:, LANES:] * full[:, LANES:]
        acc[s] += power.reshape(GROUP, radix, LANES).sum(axis=0)
        return carry

    lax.fori_loop(0, streams, transform, 0)

    def correlate(p, carry):
        a = pairs[p, 0]
        b = pairs[p, 1]
        total_re = acc[streams + p]
        total_im = acc[streams + count + p]
        for f in range(GROUP):
            span = slice(f * radix, (f + 1) * radix)
            a_re = spec[a, span, :LANES]
            a_im = spec[a, span, LANES:]
            b_re = spec[b, span, :LANES]
            b_im = spec[b, span, LANES:]
            total_re = total_re + (a_re * b_re + a_im * b_im)
            total_im = total_im + (a_im * b_re - a_re * b_im)
        acc[streams + p] = total_re
        acc[streams + count + p] = total_im
        return carry

    lax.fori_loop(0, count, correlate, 0)

    @pl.when(step == last)
    def _():
        if finish:
            for first in range(0, streams + 2 * count, per_row):
                block = acc[first : first + per_row].reshape(LANES, LANES)
                for f, piece in enumerate(natural(block, radix)):
                    sums[first + f] = piece
        else:
            sums[...] = acc[...]


def channelize(consts, acc_in, old2, old1, cur, steps, skip, finish):
    streams = cur[0].shape[0]
    rows = consts[1].shape[1]
    radix = rows // 2
    size = GROUP * rows

    def block(entry):
        array, first = entry
        return pl.BlockSpec(
            (streams, min(size, array.shape[1]), LANES), lambda i: (0, first + i, 0)
        )

    whole = pl.BlockSpec(memory_space=pltpu.VMEM)
    ins = [pl.BlockSpec(memory_space=pltpu.SMEM)] + [whole] * 5
    ins += [block(old2), block(old1), block(cur)]
    args = list(consts) + [acc_in, old2[0], old1[0], cur[0]]
    return pl.pallas_call(
        functools.partial(kernel, skip=skip, finish=finish),
        grid=(steps,),
        in_specs=ins,
        out_specs=[
            pl.BlockSpec((streams, GROUP * radix, 2 * LANES), lambda i: (0, i, 0)),
            whole,
        ],
        out_shape=[
            jax.ShapeDtypeStruct((streams, steps * GROUP * radix, 2 * LANES), jnp.float32),
            jax.ShapeDtypeStruct(acc_in.shape, jnp.float32),
        ],
        scratch_shapes=[
            pltpu.VMEM((streams, size, LANES), jnp.float32),
            pltpu.VMEM(acc_in.shape, jnp.float32),
        ],
        compiler_params=pltpu.CompilerParams(vmem_limit_bytes=58 << 20),
        name="channelize",
    )(*args)


def multiply_kernel(pairs, *refs):
    *specs, out, nat = refs
    count = pairs.shape[0]
    radix = out.shape[3] // LANES
    per_row = LANES // radix

    def work(spec):
        def correlate(p, carry):
            a = pairs[p, 0]
            b = pairs[p, 1]
            for half in range(GROUP // per_row):
                span = slice(half * LANES, (half + 1) * LANES)
                a_re = spec[a, span, :LANES]
                a_im = spec[a, span, LANES:]
                b_re = spec[b, span, :LANES]
                b_im = spec[b, span, LANES:]
                for part in range(2):
                    if part == 0:
                        prod = a_re * b_re + a_im * b_im
                    else:
                        prod = a_im * b_re - a_re * b_im
                    for f, block in enumerate(natural(prod, radix)):
                        start = (half * per_row + f) * PITCH
                        nat[part, start : start + radix, :] = block
            for part in range(2):
                for s in range(radix):
                    out[part, p, :, s * LANES : (s + 1) * LANES] = nat[
                        part, pl.ds(s, GROUP, stride=PITCH), :
                    ]
            return carry

        lax.fori_loop(0, count, correlate, 0)

    if len(specs) == 1:
        work(specs[0])
    else:
        for index, spec in enumerate(specs):
            pl.when(pl.program_id(0) == index)(functools.partial(work, spec))


def multiply(pairs, specs, channels):
    streams = specs[0].shape[0]
    radix = channels // LANES
    size = GROUP * radix
    count = pairs.shape[0]
    if len(specs) == 1:
        steps = specs[0].shape[1] // size
        ins = [pl.BlockSpec((streams, size, 2 * LANES), lambda i: (0, i, 0))]
    else:
        steps = len(specs)
        ins = [pl.BlockSpec((streams, size, 2 * LANES), lambda i: (0, 0, 0))] * steps
    return pl.pallas_call(
        multiply_kernel,
        grid=(steps,),
        in_specs=[pl.BlockSpec(memory_space=pltpu.SMEM)] + ins,
        out_specs=pl.BlockSpec((2, count, GROUP, channels), lambda i: (0, 0, i, 0)),
        out_shape=jax.ShapeDtypeStruct((2, count, steps * GROUP, channels), jnp.float32),
        scratch_shapes=[pltpu.VMEM((2, GROUP * PITCH, LANES), jnp.float32)],
        compiler_params=pltpu.CompilerParams(vmem_limit_bytes=58 << 20),
        name="multiply",
    )(pairs, *specs)


def finish_kernel(pairs, sums, out, auto, *, frames):
    count = pairs.shape[0]
    streams = sums.shape[1] - 2 * count
    mean = jnp.sum(sums[...], axis=0) / frames
    auto[...] = mean[:streams] + 1e-06
    for p in range(count):
        a = auto[pl.ds(pairs[p, 0], 1), :]
        b = auto[pl.ds(pairs[p, 1], 1), :]
        denom = a * b
        re = mean[streams + p : streams + p + 1]
        im = mean[streams + count + p : streams + count + p + 1]
        coherence = (re * re + im * im) / denom
        factor = 1.0 / jnp.sqrt(denom)
        for d in range(out.shape[0]):
            out[d, p : p + 1, :] = coherence
            out[d, count + p : count + p + 1, :] = factor


def finish_sums(pairs, sums, frames):
    devices, lines, width = sums.shape
    count = pairs.shape[0]
    whole = pl.BlockSpec(memory_space=pltpu.VMEM)
    return pl.pallas_call(
        functools.partial(finish_kernel, frames=frames),
        in_specs=[pl.BlockSpec(memory_space=pltpu.SMEM), whole],
        out_specs=whole,
        out_shape=jax.ShapeDtypeStruct((devices, 2 * count, width), jnp.float32),
        scratch_shapes=[pltpu.VMEM((lines - 2 * count, width), jnp.float32)],
        compiler_params=pltpu.CompilerParams(vmem_limit_bytes=12 << 20),
        name="finish",
    )(pairs, sums)


def scale_kernel(factor, early, late, out):
    step = pl.program_id(0)

    def scale(prod):
        for p in range(prod.shape[1]):
            out[:, p] = prod[:, p] * factor[p : p + 1, :][None]

    pl.when(step < 2)(functools.partial(scale, early))
    pl.when(step >= 2)(functools.partial(scale, late))


def rescale(early, late, factor):
    parts, count, frames, channels = late.shape
    block = (parts, count, GROUP, channels)
    total = frames + early.shape[2]
    return pl.pallas_call(
        scale_kernel,
        grid=(total // GROUP,),
        in_specs=[
            pl.BlockSpec(memory_space=pltpu.VMEM),
            pl.BlockSpec(block, lambda i: (0, 0, jnp.minimum(i, 1), 0)),
            pl.BlockSpec(block, lambda i: (0, 0, jnp.maximum(i - 2, 0), 0)),
        ],
        out_specs=pl.BlockSpec(block, lambda i: (0, 0, i, 0)),
        out_shape=jax.ShapeDtypeStruct((parts, count, total, channels), jnp.float32),
        compiler_params=pltpu.CompilerParams(vmem_limit_bytes=58 << 20),
        name="rescale",
    )(factor, early, late)


def on_device(volts, taps, pairs):
    streams, comps, local = volts.shape
    n_taps, channels = taps.shape
    count = pairs.shape[0]
    edge = n_taps - 1
    frames = local // channels
    radix = channels // LANES
    rows = comps * radix
    devices = lax.axis_size("tm")
    samples = volts.reshape(streams, comps, local // LANES, LANES)
    samples = samples.transpose(0, 2, 1, 3).reshape(streams, frames * rows, LANES)
    far, near = cut(samples, rows, edge)
    near = shifted(near, "tm", 1)
    far = shifted(far, "tm", 1)
    left, twist, right = tables(channels)
    coef = jnp.repeat(taps.reshape(n_taps, radix, LANES), comps, axis=1)
    consts = (pairs, coef, jnp.asarray(left), jnp.asarray(twist), jnp.asarray(right))
    acc = jnp.zeros((streams + 2 * count, radix, LANES), jnp.float32)
    rest = frames // GROUP - 2
    spec2, acc = channelize(consts, acc, (samples, 0), (samples, 1), (samples, 2), rest, 1, False)
    spec1, acc = channelize(consts, acc, (near, 0), (samples, 0), (samples, 1), 1, 1, False)
    spec0, acc = channelize(consts, acc, (far, 0), (near, 0), (samples, 0), 1, 0, True)
    sums = acc.reshape(streams + 2 * count, devices, channels // devices)
    sums = lax.all_to_all(sums.transpose(1, 0, 2), "tm", 0, 0)
    late = multiply(pairs, [spec2], channels)
    both = lax.all_to_all(finish_sums(pairs, sums, frames * devices), "tm", 0, 0)
    early = multiply(pairs, [spec0, spec1], channels)
    both = both.transpose(1, 0, 2).reshape(2 * count, channels)
    return (both[:count], rescale(early, late, both[count:]))


def solution(mesh):
    return jax.shard_map(
        on_device,
        mesh=mesh,
        in_specs=(P("band", None, "tm"), P(), P()),
        out_specs=(P("band", None), P(None, "band", "tm", None)),
        check_vma=False,
    )
```

```python
import functools

import jax
import jax.numpy as jnp
import numpy as np
from jax import lax
from jax.experimental import pallas as pl
from jax.experimental.pallas import tpu as pltpu
from jax.sharding import PartitionSpec as P

LANES = 128
GROUP = 8
PITCH = 40


def shifted(array, axis, by):
    devices = lax.axis_size(axis)
    pairs = [(i, i + by) for i in range(devices) if 0 <= i + by < devices]
    return lax.ppermute(array, axis, pairs)


def halves(matrix):
    matrix = np.asarray(matrix, np.float32)
    high = matrix.astype(jnp.bfloat16)
    low = (matrix - high.astype(np.float32)).astype(jnp.bfloat16)
    return high, low


@functools.lru_cache(maxsize=None)
def tables(channels):
    radix = channels // LANES
    per_row = LANES // radix
    i = np.arange(radix)
    angle = 2.0 * np.pi * ((i[:, None] * i[None, :]) % radix) / radix
    first = np.zeros((2, radix, radix, 2))
    first[0, :, :, 0] = np.cos(angle)
    first[0, :, :, 1] = np.sin(angle)
    first[1, :, :, 0] = -np.sin(angle)
    first[1, :, :, 1] = np.cos(angle)
    high, low = halves(first.reshape(2 * radix, 2 * radix))
    left = np.concatenate([high, high, low, low], axis=1)
    j = np.arange(LANES)
    twist = 2.0 * np.pi * ((i[:, None] * j[None, :]) % channels) / channels
    twist = np.stack([np.cos(twist), np.sin(twist)]).astype(np.float32)
    g = np.arange(per_row)
    s = np.arange(radix)
    b = (per_row * s[None, :] + g[:, None]).reshape(LANES)
    angle = 2.0 * np.pi * ((j[:, None] * b[None, :]) % LANES) / LANES
    cos, sin = np.cos(angle), np.sin(angle)
    second = np.block([[cos, -sin], [sin, cos]]) / np.sqrt(channels)
    high, low = halves(second)
    right = np.concatenate([high, high, low], axis=0)
    return left, twist, right


def natural(block, radix):
    turned = block.T
    per_row = LANES // radix
    return [
        jnp.concatenate(
            [turned[g * radix : (g + 1) * radix, f * radix : (f + 1) * radix] for g in range(per_row)],
            axis=1,
        )
        for f in range(per_row)
    ]


def cut_kernel(block2, block1, out):
    size = block1.shape[1]
    early = out.shape[1] - size
    out[:, :early, :] = block2[:, size - early :, :]
    out[:, early:, :] = block1[...]


def cut(samples, rows, edge):
    streams, total, lanes = samples.shape
    size = GROUP * rows
    blocks = total // size
    whole = pl.BlockSpec(memory_space=pltpu.VMEM)
    return pl.pallas_call(
        cut_kernel,
        grid=(1,),
        in_specs=[
            pl.BlockSpec((streams, size, lanes), lambda i: (0, blocks - 2, 0)),
            pl.BlockSpec((streams, size, lanes), lambda i: (0, blocks - 1, 0)),
        ],
        out_specs=whole,
        out_shape=jax.ShapeDtypeStruct((streams, edge * rows, lanes), samples.dtype),
        compiler_params=pltpu.CompilerParams(vmem_limit_bytes=58 << 20),
        name="cut",
    )(samples, samples)


def kernel(pairs, taps, left, twist, right, acc_in, *rest, head):
    *sources, spec, sums, filt, acc = rest
    streams = sources[0].shape[0]
    count = pairs.shape[0]
    n_taps, rows, _ = taps.shape
    radix = rows // 2
    step = pl.program_id(0)
    last = pl.num_programs(0) - 1
    per_row = LANES // radix
    edge = n_taps - 1
    tiles = rows // 8

    def place(w, index):
        if head:
            at = w + index * GROUP
            return (sources[0], at) if at < edge else (sources[1], at - edge)
        at = w + 2 * GROUP - edge
        return sources[at // GROUP], at % GROUP

    @pl.when(step == 0)
    def _():
        acc[...] = acc_in[...]

    def filter_tile(index, carry, which):
        s = index // tiles
        q = pl.multiple_of((index % tiles) * 8, 8)
        coef = [taps[t, pl.ds(q, 8), :] for t in range(n_taps)]
        total = [None] * GROUP
        for w in range(n_taps - 1 + GROUP):
            ref, frame = place(w, which)
            x = ref[s, pl.ds(frame * rows + q, 8), :]
            x = x.astype(jnp.float32)
            for m in range(GROUP):
                t = m + n_taps - 1 - w
                if 0 <= t < n_taps:
                    term = coef[t] * x
                    total[m] = term if total[m] is None else total[m] + term
        for m in range(GROUP):
            filt[s, pl.ds(m * rows + q, 8), :] = total[m]
        return carry

    def filter_all(which):
        lax.fori_loop(0, streams * tiles, functools.partial(filter_tile, which=which), 0)

    if head:
        for which in range(2):
            pl.when(step == which)(functools.partial(filter_all, which))
    else:
        filter_all(0)

    def transform(s, carry):
        turned = []
        for pair in range(GROUP // 2):
            columns = []
            for f in (2 * pair, 2 * pair + 1):
                x = filt[s, f * rows : (f + 1) * rows, :]
                high = x.astype(jnp.bfloat16)
                low = (x - high.astype(jnp.float32)).astype(jnp.bfloat16)
                columns.append(jnp.concatenate([high, low, high, low], axis=0))
            y = jnp.dot(
                left[...], jnp.concatenate(columns, axis=1), preferred_element_type=jnp.float32
            )
            for f in range(2):
                re = y[:radix, f * LANES : (f + 1) * LANES]
                im = y[radix:, f * LANES : (f + 1) * LANES]
                z = jnp.concatenate(
                    [re * twist[0] + im * twist[1], im * twist[0] - re * twist[1]], axis=1
                )
                turned.append(z)
        z = jnp.concatenate(turned, axis=0)
        high = z.astype(jnp.bfloat16)
        low = (z - high.astype(jnp.float32)).astype(jnp.bfloat16)
        full = jnp.dot(
            jnp.concatenate([high, low, high], axis=1),
            right[...],
            preferred_element_type=jnp.float32,
        )
        spec[s] = full
        power = full[:, :LANES] * full[:, :LANES] + full[:, LANES:] * full[:, LANES:]
        acc[s] += power.reshape(GROUP, radix, LANES).sum(axis=0)
        return carry

    lax.fori_loop(0, streams, transform, 0)

    def correlate(p, carry):
        a = pairs[p, 0]
        b = pairs[p, 1]
        total_re = acc[streams + p]
        total_im = acc[streams + count + p]
        for f in range(GROUP):
            span = slice(f * radix, (f + 1) * radix)
            a_re = spec[a, span, :LANES]
            a_im = spec[a, span, LANES:]
            b_re = spec[b, span, :LANES]
            b_im = spec[b, span, LANES:]
            total_re = total_re + (a_re * b_re + a_im * b_im)
            total_im = total_im + (a_im * b_re - a_re * b_im)
        acc[streams + p] = total_re
        acc[streams + count + p] = total_im
        return carry

    lax.fori_loop(0, count, correlate, 0)

    @pl.when(step == last)
    def _():
        if head:
            for first in range(0, streams + 2 * count, per_row):
                block = acc[first : first + per_row].reshape(LANES, LANES)
                for f, piece in enumerate(natural(block, radix)):
                    sums[first + f] = piece
        else:
            sums[...] = acc[...]


def channelize(consts, acc_in, samples, halo):
    streams, total, _ = samples.shape
    rows = consts[1].shape[1]
    radix = rows // 2
    size = GROUP * rows
    whole = pl.BlockSpec(memory_space=pltpu.VMEM)
    ins = [pl.BlockSpec(memory_space=pltpu.SMEM)] + [whole] * 5
    args = list(consts) + [acc_in]
    head = halo is not None
    if head:
        steps = 2
        ins += [
            pl.BlockSpec(halo.shape, lambda i: (0, 0, 0)),
            pl.BlockSpec((streams, 2 * size, LANES), lambda i: (0, 0, 0)),
        ]
        args += [halo, samples]
    else:
        steps = total // size - 2
        for shift in range(3):
            ins.append(
                pl.BlockSpec((streams, size, LANES), functools.partial(lambda d, i: (0, i + d, 0), shift))
            )
            args.append(samples)
    return pl.pallas_call(
        functools.partial(kernel, head=head),
        grid=(steps,),
        in_specs=ins,
        out_specs=[
            pl.BlockSpec((streams, GROUP * radix, 2 * LANES), lambda i: (0, i, 0)),
            whole,
        ],
        out_shape=[
            jax.ShapeDtypeStruct((streams, steps * GROUP * radix, 2 * LANES), jnp.float32),
            jax.ShapeDtypeStruct(acc_in.shape, jnp.float32),
        ],
        scratch_shapes=[
            pltpu.VMEM((streams, size, LANES), jnp.float32),
            pltpu.VMEM(acc_in.shape, jnp.float32),
        ],
        compiler_params=pltpu.CompilerParams(vmem_limit_bytes=58 << 20),
        name="channelize",
    )(*args)


def multiply_kernel(pairs, spec, out, nat):
    count = pairs.shape[0]
    radix = out.shape[3] // LANES
    per_row = LANES // radix

    def correlate(p, carry):
        a = pairs[p, 0]
        b = pairs[p, 1]
        for half in range(GROUP // per_row):
            span = slice(half * LANES, (half + 1) * LANES)
            a_re = spec[a, span, :LANES]
            a_im = spec[a, span, LANES:]
            b_re = spec[b, span, :LANES]
            b_im = spec[b, span, LANES:]
            for part in range(2):
                if part == 0:
                    prod = a_re * b_re + a_im * b_im
                else:
                    prod = a_im * b_re - a_re * b_im
                for f, block in enumerate(natural(prod, radix)):
                    start = (half * per_row + f) * PITCH
                    nat[part, start : start + radix, :] = block
        for part in range(2):
            for s in range(radix):
                out[part, p, :, s * LANES : (s + 1) * LANES] = nat[
                    part, pl.ds(s, GROUP, stride=PITCH), :
                ]
        return carry

    lax.fori_loop(0, count, correlate, 0)


def multiply(pairs, spectra, channels):
    streams = spectra.shape[0]
    size = GROUP * (channels // LANES)
    count = pairs.shape[0]
    steps = spectra.shape[1] // size
    ins = [pl.BlockSpec((streams, size, 2 * LANES), lambda i: (0, i, 0))]
    return pl.pallas_call(
        multiply_kernel,
        grid=(steps,),
        in_specs=[pl.BlockSpec(memory_space=pltpu.SMEM)] + ins,
        out_specs=pl.BlockSpec((2, count, GROUP, channels), lambda i: (0, 0, i, 0)),
        out_shape=jax.ShapeDtypeStruct((2, count, steps * GROUP, channels), jnp.float32),
        scratch_shapes=[pltpu.VMEM((2, GROUP * PITCH, LANES), jnp.float32)],
        compiler_params=pltpu.CompilerParams(vmem_limit_bytes=58 << 20),
        name="multiply",
    )(pairs, spectra)


def finish_kernel(pairs, sums, after, out, auto, *, frames):
    count = pairs.shape[0]
    streams = sums.shape[1] - 2 * count
    mean = jnp.sum(sums[...], axis=0) / frames
    auto[...] = mean[:streams] + 1e-06
    for p in range(count):
        a = auto[pl.ds(pairs[p, 0], 1), :]
        b = auto[pl.ds(pairs[p, 1], 1), :]
        denom = a * b
        re = mean[streams + p : streams + p + 1]
        im = mean[streams + count + p : streams + count + p + 1]
        coherence = (re * re + im * im) / denom
        factor = 1.0 / jnp.sqrt(denom)
        for d in range(out.shape[0]):
            out[d, p : p + 1, :] = coherence
            out[d, count + p : count + p + 1, :] = factor


def finish_sums(pairs, sums, after, frames):
    devices, lines, width = sums.shape
    count = pairs.shape[0]
    whole = pl.BlockSpec(memory_space=pltpu.VMEM)
    return pl.pallas_call(
        functools.partial(finish_kernel, frames=frames),
        in_specs=[pl.BlockSpec(memory_space=pltpu.SMEM), whole, pl.BlockSpec(memory_space=pltpu.HBM)],
        out_specs=whole,
        out_shape=jax.ShapeDtypeStruct((devices, 2 * count, width), jnp.float32),
        scratch_shapes=[pltpu.VMEM((lines - 2 * count, width), jnp.float32)],
        compiler_params=pltpu.CompilerParams(vmem_limit_bytes=12 << 20),
        name="finish",
    )(pairs, sums, after)


def scale_kernel(factor, early, late, out):
    step = pl.program_id(0)

    def scale(prod):
        for p in range(prod.shape[1]):
            out[:, p] = prod[:, p] * factor[p : p + 1, :][None]

    pl.when(step < 2)(functools.partial(scale, early))
    pl.when(step >= 2)(functools.partial(scale, late))


def rescale(early, late, factor):
    parts, count, frames, channels = late.shape
    block = (parts, count, GROUP, channels)
    total = frames + early.shape[2]
    return pl.pallas_call(
        scale_kernel,
        grid=(total // GROUP,),
        in_specs=[
            pl.BlockSpec(memory_space=pltpu.VMEM),
            pl.BlockSpec(block, lambda i: (0, 0, jnp.minimum(i, 1), 0)),
            pl.BlockSpec(block, lambda i: (0, 0, jnp.maximum(i - 2, 0), 0)),
        ],
        out_specs=pl.BlockSpec(block, lambda i: (0, 0, i, 0)),
        out_shape=jax.ShapeDtypeStruct((parts, count, total, channels), jnp.float32),
        compiler_params=pltpu.CompilerParams(vmem_limit_bytes=58 << 20),
        name="rescale",
    )(factor, early, late)


def on_device(volts, taps, pairs):
    streams, comps, local = volts.shape
    n_taps, channels = taps.shape
    count = pairs.shape[0]
    edge = n_taps - 1
    frames = local // channels
    radix = channels // LANES
    rows = comps * radix
    devices = lax.axis_size("tm")
    samples = volts.reshape(streams, comps, local // LANES, LANES)
    samples = samples.transpose(0, 2, 1, 3).reshape(streams, frames * rows, LANES)
    halo = shifted(cut(samples, rows, edge), "tm", 1)
    left, twist, right = tables(channels)
    coef = jnp.repeat(taps.reshape(n_taps, radix, LANES), comps, axis=1)
    consts = (pairs, coef, jnp.asarray(left), jnp.asarray(twist), jnp.asarray(right))
    acc = jnp.zeros((streams + 2 * count, radix, LANES), jnp.float32)
    spec_late, acc = channelize(consts, acc, samples, None)
    spec_early, acc = channelize(consts, acc, samples, halo)
    sums = acc.reshape(streams + 2 * count, devices, channels // devices)
    sums = lax.all_to_all(sums.transpose(1, 0, 2), "tm", 0, 0)
    late = multiply(pairs, spec_late, channels)
    both = lax.all_to_all(finish_sums(pairs, sums, late[0, 0, :GROUP, :LANES], frames * devices), "tm", 0, 0)
    early = multiply(pairs, spec_early, channels)
    both = both.transpose(1, 0, 2).reshape(2 * count, channels)
    return (both[:count], rescale(early, late, both[count:]))


def solution(mesh):
    return jax.shard_map(
        on_device,
        mesh=mesh,
        in_specs=(P("band", None, "tm"), P(), P()),
        out_specs=(P("band", None), P(None, "band", "tm", None)),
        check_vma=False,
    )
```
